32 devices in a mesh: xfer: 8 (over y, x, core), head: 4 (over z).
Axes of the slice: x: 2, y: 2, z: 4, core: 2. Of those that a mesh axis runs over, the one named last changes fastest.
Arguments:
- kv_pool: bfloat16 [256, 64, 576], P(('xfer', 'head')), may hold values from -8 to 8
- lengths: int32 [64], replicated, may hold values from 2 to 1600, as said below
- start_device: int32 [64], replicated, may hold values from 0 to 31, as said below
- page_table: int32 [64, 32], replicated, may hold values from 0 to 7, as said below
- queries: bfloat16 [128, 128, 192], P('xfer', 'head'), may hold values from -100 to 100
- new_latent: bfloat16 [128, 576], P('xfer'), may hold values from -100 to 100
- key_up: bfloat16 [128, 128, 512], P('head'), may hold values from -0.25 to 0.25
- value_up: bfloat16 [128, 512, 128], P('head'), may hold values from -0.25 to 0.25
- out_proj: bfloat16 [16384, 7168], P('head', 'xfer'), may hold values from -0.046875 to 0.046875
Outputs:
- attn_out: bfloat16 [128, 7168], P('head', 'xfer')
The draws below stay inside these ranges and needn't reach their ends.
Inputs may be any that keep to these rules, and one draw needn't show every extreme that they name: `lengths`: request r belongs to decode owner xfer index r // 8. The pages of one owner's requests number 32 // 2 to 32, exactly 32 for some owner, so one owner has at most one page on any device. Page j of request r lies on device (start_device[r] + j) mod 32. `page_table`: entries past a request's pages are 0; two pages on one device never share a slot.
All inputs are finite; a program needn't handle non-finite values.
Results may differ from the reference program's by a relative error of at most 0.0058.
Values may be sent and summed in bfloat16 or wider, within the bound.
No kernel may reach another device: no remote copies, remote signals or barrier semaphores. Data moves between devices by JAX's collectives and lax.ppermute only.
A program may use at most 128 MiB of HBM per device.

```python
import jax
import jax.numpy as jnp
from jax import lax

D_MODEL = 7168
HEADS = 128
NOPE = 128
LAT_RANK = 512
VDIM = 128
PAGE = 64
STEPS = 2
R_DEV = 8
QDIM = 192
LAT = 576
REQUESTS = 64
ROWS = 128
MAXP = 32
POOL = 256
N_XFER = 8
DEVICES = 32


def layout(key):
    key_total = jax.random.fold_in(key, 11)
    key_force = jax.random.fold_in(key, 12)
    key_split = jax.random.fold_in(key, 13)
    key_trim = jax.random.fold_in(key, 14)
    key_base = jax.random.fold_in(key, 15)
    key_shuffle = jax.random.fold_in(key, 16)
    key_longest = jax.random.fold_in(key, 17)
    totals = jax.random.randint(key_total, (N_XFER,), DEVICES // 2, DEVICES + 1)
    forced = jax.random.randint(key_force, (), 0, N_XFER)
    totals = jnp.where(jnp.arange(N_XFER) == forced, DEVICES, totals).astype(jnp.int32)
    positions = jnp.arange(1, DEVICES, dtype=jnp.int32)
    jitter = jax.random.randint(key_split, (N_XFER, DEVICES - 1), 0, 1 << 20)
    ranked = jnp.where(positions[None, :] < totals[:, None], jitter * DEVICES + positions[None, :], -1 - positions[None, :])
    cut_points, _ = lax.top_k(ranked, R_DEV - 1)
    cut_points = jnp.sort(cut_points % DEVICES, axis=1)
    boundary = jnp.concatenate([jnp.zeros((N_XFER, 1), jnp.int32), cut_points, totals[:, None]], axis=1)
    page_counts = boundary[:, 1:] - boundary[:, :-1]
    longest_slot = jax.random.randint(key_longest, (), 0, R_DEV)
    request_slot = jnp.arange(R_DEV, dtype=jnp.int32)
    special = jnp.where(request_slot == longest_slot, DEVICES - R_DEV + 1, 1).astype(jnp.int32)
    owner_rows = jnp.arange(N_XFER, dtype=jnp.int32)
    page_counts = jnp.where(owner_rows[:, None] == forced, special[None, :], page_counts).astype(jnp.int32)
    offsets = jnp.cumsum(page_counts, axis=1) - page_counts
    base_device = jax.random.randint(key_base, (N_XFER, 1), 0, DEVICES)
    start_dev = ((base_device + offsets) % DEVICES).reshape(REQUESTS).astype(jnp.int32)
    flat_counts = page_counts.reshape(REQUESTS)
    trimmed = jax.random.randint(key_trim, (REQUESTS,), 0, PAGE - 1)
    longest_request = forced * R_DEV + longest_slot
    trimmed = jnp.where(jnp.arange(REQUESTS, dtype=jnp.int32) == longest_request, 0, trimmed)
    length_all = (flat_counts * PAGE - trimmed).astype(jnp.int32)
    subkeys = jax.random.split(key_shuffle, DEVICES)
    shuffle = jax.vmap(lambda subkey: jax.random.permutation(subkey, N_XFER))(subkeys).astype(jnp.int32)
    owner_of = jnp.arange(REQUESTS, dtype=jnp.int32) // R_DEV
    column = jnp.arange(MAXP, dtype=jnp.int32)
    device_of = (start_dev[:, None] + column[None, :]) % DEVICES
    page_slots = shuffle[device_of, owner_of[:, None]]
    page_slots = jnp.where(column[None, :] < flat_counts[:, None], page_slots, 0).astype(jnp.int32)
    return (length_all, start_dev, page_slots)


def draw_lengths(key, part):
    return layout(key)[0]


def draw_start_device(key, part):
    return layout(key)[1]


def draw_page_table(key, part):
    return layout(key)[2]


def draw_kv_pool(key, part):
    key_pool = jax.random.fold_in(key, 201)
    pool = jnp.clip(jax.random.normal(key_pool, (POOL, PAGE, LAT), jnp.float32), -6.0, 6.0)
    return pool.astype(jnp.bfloat16)


def drawn(key):
    key_fresh = jax.random.fold_in(key, 101)
    key_query = jax.random.fold_in(key, 102)
    key_pull = jax.random.fold_in(key, 103)
    fresh_rows = jax.random.normal(key_fresh, (ROWS, LAT), jnp.float32)
    base_query = jax.random.normal(key_query, (ROWS, HEADS, QDIM), jnp.float32)
    strengths = jax.random.uniform(key_pull, (ROWS, HEADS), jnp.float32, 0.5, 2.0)
    rope_rows = fresh_rows[:, LAT_RANK:]
    query_rope = base_query[:, :, NOPE:] + strengths[:, :, None] * rope_rows[:, None, :]
    full_query = jnp.concatenate([base_query[:, :, :NOPE], query_rope], axis=-1)
    return (full_query, fresh_rows)


def draw_queries(key, part):
    return drawn(key)[0].astype(jnp.bfloat16)


def draw_new_latent(key, part):
    return drawn(key)[1].astype(jnp.bfloat16)


def block_levels(own_key, shape, shards, smallest, top_value):
    factor_of, own = 1.0, jax.random.fold_in(own_key, 6)
    for position, shards_of in shards:
        draws = jnp.exp(jax.random.uniform(jax.random.fold_in(own, position), (shards_of,), jnp.float32, smallest / len(shards), top_value / len(shards)))
        factor_of = factor_of * jnp.repeat(draws, shape[position] // shards_of).reshape([-1 if axis == position else 1 for axis in range(len(shape))])
    return factor_of


def centred(rng, shape, deviation, bound, cuts=(), held_as=jnp.bfloat16):
    entries = jax.random.normal(rng, shape, jnp.float32) * deviation
    if len(cuts) > 0:
        entries = block_levels(rng, shape, cuts, -0.22, 0.18) * entries
    return jnp.clip(entries, min=-bound, max=bound).astype(held_as)


def setup_inputs(seed: int = 0) -> dict:
    streams_of = jax.random.split(jax.random.key(seed), 10)
    return {
        "kv_pool": draw_kv_pool(jax.random.fold_in(streams_of[9], 71), 0),
        "lengths": draw_lengths(jax.random.fold_in(streams_of[9], 71), 0),
        "start_device": draw_start_device(jax.random.fold_in(streams_of[9], 71), 0),
        "page_table": draw_page_table(jax.random.fold_in(streams_of[9], 71), 0),
        "queries": draw_queries(jax.random.fold_in(streams_of[9], 71), 0),
        "new_latent": draw_new_latent(jax.random.fold_in(streams_of[9], 71), 0),
        "key_up": centred(streams_of[6], (HEADS, NOPE, LAT_RANK), LAT_RANK ** -0.5, 0.25, ((0, 4),)),
        "value_up": centred(streams_of[7], (HEADS, LAT_RANK, VDIM), LAT_RANK ** -0.5, 0.25, ((0, 4),)),
        "out_proj": centred(streams_of[8], (HEADS * VDIM, D_MODEL), (HEADS * VDIM) ** -0.5, 0.046875, ((0, 4), (1, 8))),
    }


def reference(kv_pool, lengths, start_device, page_table, queries, new_latent, key_up, value_up, out_proj):
    score_scale = QDIM ** -0.5
    page_index = jnp.arange(MAXP, dtype=jnp.int32)
    absorbed = jnp.einsum("rhn,hnc->rhc", queries[:, :, :NOPE].astype(jnp.float32), key_up.astype(jnp.float32)).astype(jnp.bfloat16)
    qfull = jnp.concatenate([absorbed, queries[:, :, NOPE:]], axis=-1)
    qfull = qfull.reshape(REQUESTS, STEPS, HEADS, LAT)
    fresh_rows = new_latent.reshape(REQUESTS, STEPS, LAT)
    step_index = jnp.arange(STEPS, dtype=jnp.int32)
    causal = step_index[:, None] >= step_index[None, :]

    def per_request(inputs):
        length, first, slot_row, query_rows, fresh = inputs
        device_of = (first + page_index) % DEVICES
        pool_index = (device_of * N_XFER + slot_row).astype(jnp.int32)
        key_rows = kv_pool[pool_index].reshape(MAXP * PAGE, LAT).astype(jnp.float32)
        visible = jnp.arange(MAXP * PAGE, dtype=jnp.int32) < length
        query_f = query_rows.astype(jnp.float32)
        fresh_f = fresh.astype(jnp.float32)
        cached = jnp.einsum("thc,kc->thk", query_f, key_rows) * score_scale
        cached = jnp.where(visible[None, None, :], cached, -jnp.inf)
        recent = jnp.einsum("thc,kc->thk", query_f, fresh_f) * score_scale
        recent = jnp.where(causal[:, None, :], recent, -jnp.inf)
        row_top = jnp.maximum(jnp.max(cached, axis=-1), jnp.max(recent, axis=-1))
        cached_w = jnp.exp(cached - row_top[..., None])
        recent_w = jnp.exp(recent - row_top[..., None])
        total = jnp.sum(cached_w, axis=-1) + jnp.sum(recent_w, axis=-1)
        summed = jnp.einsum("thk,kc->thc", cached_w.astype(jnp.bfloat16).astype(jnp.float32), key_rows[:, :LAT_RANK])
        summed = summed + jnp.einsum("thk,kc->thc", recent_w.astype(jnp.bfloat16).astype(jnp.float32), fresh_f[:, :LAT_RANK])
        return (summed / total[..., None]).astype(jnp.bfloat16)

    latent_out = lax.map(per_request, (lengths, start_device, page_table, qfull, fresh_rows))
    latent_out = latent_out.reshape(ROWS, HEADS, LAT_RANK)
    head_out = jnp.einsum("rhc,hcv->rhv", latent_out.astype(jnp.float32), value_up.astype(jnp.float32)).astype(jnp.bfloat16)
    head_out = head_out.reshape(ROWS, HEADS * VDIM)
    return jnp.dot(head_out, out_proj, preferred_element_type=jnp.float32).astype(jnp.bfloat16)
```

```python
import functools

import jax
import jax.numpy as jnp
from jax import lax
from jax.experimental import pallas as pl
from jax.experimental.pallas import tpu as pltpu
from jax.sharding import PartitionSpec as P


STEPS = 2
HIDDEN = -1e30
F32 = jnp.float32
BF16 = jnp.bfloat16
ANY = pl.BlockSpec(memory_space=pl.ANY)
HBM = pl.BlockSpec(memory_space=pltpu.HBM)
VMEM = pl.BlockSpec(memory_space=pltpu.VMEM)
SMEM = pl.BlockSpec(memory_space=pltpu.SMEM)


def gather_kernel(cfg, idx, lengths_hbm, starts_hbm, table_hbm, pool_hbm, other, same, *scratch):
    devices, groups, per_owner = cfg
    lengths, starts, table, pool, sem = scratch
    copies = [
        pltpu.make_async_copy(src, dst, sem.at[i])
        for i, (src, dst) in enumerate(
            ((lengths_hbm, lengths), (starts_hbm, starts), (table_hbm, table), (pool_hbm, pool))
        )
    ]
    for c in copies:
        c.start()
    page_len = pool.shape[1]
    half = other.shape[0]
    me, z = idx[0], idx[1]
    column = lax.broadcasted_iota(jnp.int32, table.shape, 0)
    request = lax.broadcasted_iota(jnp.int32, table.shape, 1)
    for c in copies[:3]:
        c.wait()
    at = starts[...] + column
    here = jnp.where(at >= devices, at - devices, at) == me * groups + z
    here = here & (column * page_len < lengths[...])
    slots = jnp.where(here, table[...], 0)
    owner = request // per_owner
    chosen = []
    for flip in (1, 0):
        for m in range(half):
            chosen.append(jnp.sum(jnp.where(owner == me ^ (2 * m) ^ flip, slots, 0)))
    copies[3].wait()
    for m in range(half):
        other[m] = pool[chosen[m]]
        same[m] = pool[chosen[half + m]]


def gather_pages(idx, pool, lengths, starts, table, groups):
    requests, _ = table.shape
    owners = pool.shape[0]
    half = jax.ShapeDtypeStruct((owners // 2,) + pool.shape[1:], pool.dtype)
    cfg = (owners * groups, groups, requests // owners)
    args = (lengths.reshape(1, -1), starts.reshape(1, -1), table.T, pool)
    args = tuple(pltpu.with_memory_space_constraint(x, pltpu.HBM) for x in args)
    return pl.pallas_call(
        functools.partial(gather_kernel, cfg),
        out_shape=[half] * 2,
        in_specs=[SMEM] + [HBM] * 4,
        out_specs=[VMEM] * 2,
        scratch_shapes=[pltpu.VMEM(x.shape, x.dtype) for x in args]
        + [pltpu.SemaphoreType.DMA((4,))],
        compiler_params=pltpu.CompilerParams(vmem_limit_bytes=16 << 20),
    )(idx, *args)


def pack_kernel(same, part, ring, *outs):
    last = len(outs)
    for i, source in enumerate((same, part)):
        ring[i] = source[0]
        ring[2 + i] = source[last]
        for m, out in enumerate(outs, 1):
            out[i] = source[m]


def pack_pages(same, part):
    pair = jax.ShapeDtypeStruct((2,) + same.shape[1:], same.dtype)
    ring = jax.ShapeDtypeStruct((4,) + same.shape[1:], same.dtype)
    count = same.shape[0] - 1
    return pl.pallas_call(
        pack_kernel,
        out_shape=[ring] + [pair] * count,
        in_specs=[VMEM] * 2,
        out_specs=[VMEM] * (count + 1),
        compiler_params=pltpu.CompilerParams(vmem_limit_bytes=16 << 20),
    )(same, part)


def absorb_kernel(queries_hbm, key_up_hbm, out, queries, key_up, flat, rope, sem):
    rows, heads, dim = queries.shape
    nope, rank = key_up.shape[1:]
    pieces = sem.shape[0] - 1
    n = heads // pieces
    copies = [pltpu.make_async_copy(queries_hbm, queries, sem.at[pieces])]
    for i in range(pieces):
        at = pl.ds(i * n, n)
        copies.append(pltpu.make_async_copy(key_up_hbm.at[at], key_up.at[at], sem.at[i]))
    for c in copies:
        c.start()
    copies[0].wait()
    q = queries[...].reshape(rows * heads, dim).astype(F32)
    flat[...] = q[:, :nope]
    rope[:, : dim - nope] = q[:, nope:]
    for h in range(heads):
        if h % n == 0:
            copies[1 + h // n].wait()
        pick = pl.ds(h, rows, stride=heads)
        at = pl.ds(h * rows, rows)
        out[at, :rank] = jnp.dot(
            flat[pick, :].astype(BF16), key_up[h], preferred_element_type=F32
        ).astype(BF16)
        out[at, rank:] = rope[pick, :][:, : dim - nope].astype(BF16)


def absorb(queries, key_up):
    rows, heads, dim = queries.shape
    width = key_up.shape[2] + dim - key_up.shape[1]
    args = tuple(pltpu.with_memory_space_constraint(x, pltpu.HBM) for x in (queries, key_up))
    return pl.pallas_call(
        absorb_kernel,
        out_shape=jax.ShapeDtypeStruct((heads * rows, width), BF16),
        in_specs=[HBM] * 2,
        out_specs=VMEM,
        scratch_shapes=[
            pltpu.VMEM(queries.shape, queries.dtype),
            pltpu.VMEM(key_up.shape, key_up.dtype),
            pltpu.VMEM((rows * heads, key_up.shape[1]), F32),
            pltpu.VMEM((rows * heads, pl.cdiv(dim - key_up.shape[1], 128) * 128), F32),
            pltpu.SemaphoreType.DMA((5,)),
        ],
        compiler_params=pltpu.CompilerParams(vmem_limit_bytes=16 << 20),
        cost_estimate=pl.CostEstimate(
            flops=2 * rows * key_up.size, transcendentals=0, bytes_accessed=2 * key_up.size
        ),
    )(*args)


def row_chunks(heads, rows):
    size = max(1, 512 // rows)
    return [(h, min(size, heads - h)) for h in range(0, heads, size)]


def attend(q, parts, scale, lat_rank, old):
    n = q.shape[0]
    scores = []
    for keys, bias in parts:
        rows = bias.shape[0]
        s = lax.dot_general(q, keys, (((1,), (1,)), ((), ())), preferred_element_type=F32)
        scores.append((s.reshape(n // rows, rows, -1) * scale + bias[None]).reshape(n, -1))
    m = functools.reduce(jnp.maximum, [jnp.max(s, axis=-1, keepdims=True) for s in scores])
    if old is not None:
        m = jnp.maximum(old[0], m)
    l, acc = 0.0, 0.0
    for s, (keys, _) in zip(scores, parts):
        w = jnp.exp(s - m)
        l = l + jnp.sum(w, axis=-1, keepdims=True)
        acc = acc + jnp.dot(w.astype(BF16), keys[:, :lat_rank], preferred_element_type=F32)
    if old is not None:
        keep = jnp.exp(old[0] - m)
        l = l + old[1] * keep
        acc = acc + old[2] * keep
    return m, l, acc


def fill_bias(cfg, idx, lengths, starts, bias):
    devices, groups, per_owner, page_len = cfg
    rows, width = bias.shape[1:]
    tile = max(128, page_len)
    lane = lax.broadcasted_iota(jnp.int32, (rows, tile), 1)
    request = lax.broadcasted_iota(jnp.int32, (rows, tile), 0) // STEPS
    me = idx[0]

    def one(i, _):
        plane, t = i // (width // tile), lax.rem(i, width // tile)
        limit = jnp.zeros((rows, tile), jnp.int32)
        for p in range(tile // page_len):
            home = (me ^ (t * (tile // page_len) + p)) * groups + plane
            for r in range(per_owner):
                at = home - starts[me * per_owner + r]
                at = jnp.where(at < 0, at + devices, at)
                seen = lengths[me * per_owner + r] - (at - p) * page_len
                limit = jnp.where((request == r) & (lane // page_len == p), seen, limit)
        bias[plane, :, pl.ds(pl.multiple_of(t * tile, tile), tile)] = jnp.where(
            lane < limit, 0.0, HIDDEN
        ).astype(F32)
        return 0

    lax.fori_loop(0, groups * (width // tile), one, 0)


def stage_kernel(cfg, *rest):
    heads, rows, lat_rank, scale, counts, first, last, hops, geometry, skips = cfg
    rest = list(rest)

    def take(n):
        out = rest[:n]
        del rest[:n]
        return out

    idx, q = take(2)
    if first:
        lengths, starts, fresh = take(3)
    else:
        bias, m_in, l_in, acc_in = take(4)
    if last:
        (value_up,) = take(1)
    blocks = [list(zip(take(len(c)), c)) for c in counts]
    if last:
        (out,) = take(1)
    else:
        m_s, l_s, acc_s = take(3)
    if first:
        (bias,) = take(1)
        fill_bias(geometry, idx, lengths, starts, bias)
    groups = geometry[1]
    z = idx[1]
    parts = []
    if first:
        row = lax.broadcasted_iota(jnp.int32, (rows, rows), 0)
        col = lax.broadcasted_iota(jnp.int32, (rows, rows), 1)
        ok = (row // STEPS == col // STEPS) & (col <= row)
        parts.append((fresh[...], jnp.where(ok, 0.0, HIDDEN).astype(F32)))
    for hop, skip, block in zip(hops, skips, blocks):
        plane = lax.rem(z + groups - hop, groups)
        at = skip
        for ref, pages in block:
            n = pages * ref.shape[1]
            parts.append((ref[:pages].reshape(n, -1), bias[plane, :, at : at + n]))
            at += n
    for h, n in row_chunks(heads, rows):
        at = pl.ds(h * rows, n * rows)
        old = None if first else (m_in[at], l_in[at], acc_in[at])
        m, l, acc = attend(q[at], parts, scale, lat_rank, old)
        if last:
            latent = (acc * (1.0 / l)).astype(BF16).reshape(n, rows, lat_rank)
            vdim = value_up.shape[-1]
            for i in range(n):
                o = jnp.dot(latent[i], value_up[h + i], preferred_element_type=F32)
                out[:, (h + i) * vdim : (h + i + 1) * vdim] = o.astype(BF16)
        else:
            m_s[at], l_s[at], acc_s[at] = m, l, acc


def stage(
    idx, q, blocks, hops, dims, geometry, fresh=None, state=None, value_up=None, skips=(0, 0)
):
    heads, rows, lat_rank, scale = dims
    first, last = fresh is not None, value_up is not None
    args, specs = [idx, q], [SMEM, VMEM]
    if first:
        args += list(fresh)
        specs += [SMEM, SMEM, VMEM]
    else:
        args += list(state)
        specs += [VMEM] * 4
    if last:
        args.append(value_up)
        specs.append(VMEM)
    for block in blocks:
        args += [x for x, _ in block]
        specs += [VMEM] * len(block)
    tokens = sum(n for _, n in blocks[0]) * geometry[3]
    total = sum(n for b in blocks for _, n in b) * geometry[3]
    if last:
        out_shape = jax.ShapeDtypeStruct((rows, heads * value_up.shape[2]), BF16)
        out_specs = VMEM
    else:
        out_shape = [
            jax.ShapeDtypeStruct((heads * rows, 1), F32),
            jax.ShapeDtypeStruct((heads * rows, 1), F32),
            jax.ShapeDtypeStruct((heads * rows, lat_rank), F32),
        ]
        if first:
            out_shape.append(jax.ShapeDtypeStruct((geometry[1], rows, tokens), F32))
        out_specs = [VMEM] * len(out_shape)
    cfg = (
        heads, rows, lat_rank, scale, tuple(tuple(n for _, n in b) for b in blocks), first, last, tuple(hops),
        geometry, skips,
    )
    work = 2 * heads * rows * total * (q.shape[1] + lat_rank)
    return pl.pallas_call(
        functools.partial(stage_kernel, cfg),
        out_shape=out_shape,
        in_specs=specs,
        out_specs=out_specs,
        compiler_params=pltpu.CompilerParams(vmem_limit_bytes=24 << 20),
        cost_estimate=pl.CostEstimate(flops=work, transcendentals=0, bytes_accessed=4 << 20),
    )(*args)


def project_kernel(masks, groups, idx, *rest):
    blocks = rest[: len(masks)]
    w = rest[len(masks)]
    outs = rest[len(masks) + 1 : len(masks) + 1 + groups]
    lhs, acc = rest[len(masks) + 1 + groups :]
    rows = blocks[0].shape[0]
    cols = w.shape[1]
    me, z = idx[0], idx[1]
    for mask, block in zip(masks, blocks):
        lhs[pl.ds(pl.multiple_of((me ^ mask) * rows, rows), rows)] = block[...]
    for c in range(0, cols, 256):
        n = min(256, cols - c)
        acc[:, c : c + n] = jnp.dot(lhs[...], w[:, c : c + n], preferred_element_type=F32)
        for j, out in enumerate(outs):
            k = out.shape[0]
            at = pl.multiple_of((z ^ j) * k, k)
            out[:, c : c + n] = acc[pl.ds(at, k), c : c + n].astype(out.dtype)


def project(idx, masks, blocks, w, groups):
    rows, depth = blocks[0].shape
    total = rows * len(blocks)
    cols = w.shape[1]
    chunk = total // groups
    outs = [jax.ShapeDtypeStruct((chunk, cols), F32 if j == 0 else BF16) for j in range(groups)]
    return pl.pallas_call(
        functools.partial(project_kernel, tuple(masks), groups),
        out_shape=outs,
        in_specs=[SMEM] + [VMEM] * (len(blocks) + 1),
        out_specs=[VMEM] * groups,
        scratch_shapes=[
            pltpu.VMEM((total, depth), BF16),
            pltpu.VMEM((total, cols), F32),
        ],
        compiler_params=pltpu.CompilerParams(vmem_limit_bytes=24 << 20),
        cost_estimate=pl.CostEstimate(
            flops=2 * total * depth * cols, transcendentals=0, bytes_accessed=2 * depth * cols
        ),
    )(idx, *blocks, w)


def swap_x(x, mask, owners):
    return lax.ppermute(x, "xfer", [(i, i ^ mask) for i in range(owners)])


def shift_z(x, k, groups):
    return lax.ppermute(x, "head", [(i, (i + k) % groups) for i in range(groups)])


def whole(
    kv_pool, lengths, start_device, page_table, queries, new_latent, key_up, value_up, out_proj
):
    owners = lax.axis_size("xfer")
    groups = lax.axis_size("head")
    page_len = kv_pool.shape[1]
    lat_rank = value_up.shape[1]
    heads = key_up.shape[0]
    rows = queries.shape[0]
    idx = jnp.stack([lax.axis_index("xfer"), lax.axis_index("head")])

    other, same = gather_pages(idx, kv_pool, lengths, start_device, page_table, groups)
    part = swap_x(other, 1, owners)
    ring, *sent, side = pack_pages(same, part)
    far = jnp.concatenate([swap_x(x, 2 * m, owners) for m, x in enumerate(sent, 1)], axis=0)
    across = owners - 2
    hops = [(ring, far, swap_x(side, across, owners))]
    for _ in range(groups - 1):
        ring = shift_z(ring, 1, groups)
        far = shift_z(far, 1, groups)
        hops.append((ring, far, swap_x(ring[2:], across, owners)))
    hops = [[(r, 2), (f, f.shape[0]), (s, 2)] for r, f, s in hops]

    q = absorb(queries, key_up)

    dims = (heads, rows, lat_rank, queries.shape[2] ** (-0.5))
    geometry = (owners * groups, groups, lengths.shape[0] // owners, page_len)
    *state, bias = stage(
        idx, q, hops[:1], (0,), dims, geometry, fresh=(lengths, start_device, new_latent)
    )
    end = groups - 1
    for t in range(1, end):
        state = stage(idx, q, [hops[t]], (t,), dims, geometry, state=[bias, *state])
    early, *late = hops[end]
    state = stage(idx, q, [[early]], (end,), dims, geometry, state=[bias, *state])
    head_out = stage(
        idx, q, [late], (end,), dims, geometry, state=[bias, *state],
        value_up=value_up, skips=(2 * page_len,),
    )

    gathered = {}
    for k in range(0, owners, 2):
        gathered[k] = swap_x(head_out, k, owners) if k else head_out
        gathered[k + 1] = swap_x(gathered[k], 1, owners)
    masks = list(range(owners))
    parts = project(idx, masks, [gathered[k] for k in masks], out_proj, groups)
    total = parts[0]
    for k in range(1, groups):
        moved = lax.ppermute(parts[k], "head", [(i, i ^ k) for i in range(groups)])
        total = total + moved.astype(F32)
    return total.astype(BF16)


def solution(mesh):
    in_specs = (
        P(("xfer", "head"), None, None),
        P(),
        P(),
        P(),
        P("xfer", "head", None),
        P("xfer", None),
        P("head", None, None),
        P("head", None, None),
        P("head", "xfer"),
    )
    out_specs = P("head", "xfer")
    return jax.shard_map(whole, mesh=mesh, in_specs=in_specs, out_specs=out_specs, check_vma=False)
```

```python
import functools

import jax
import jax.numpy as jnp
from jax import lax
from jax.experimental import pallas as pl
from jax.experimental.pallas import tpu as pltpu
from jax.sharding import PartitionSpec as P


STEPS = 2
HIDDEN = -1e30
F32 = jnp.float32
BF16 = jnp.bfloat16
ANY = pl.BlockSpec(memory_space=pl.ANY)
HBM = pl.BlockSpec(memory_space=pltpu.HBM)
VMEM = pl.BlockSpec(memory_space=pltpu.VMEM)
SMEM = pl.BlockSpec(memory_space=pltpu.SMEM)


def gather_kernel(cfg, idx, lengths_hbm, starts_hbm, table_hbm, pool_hbm, other, same, *scratch):
    devices, groups, per_owner = cfg
    lengths, starts, table, pool, sem = scratch
    copies = [
        pltpu.make_async_copy(src, dst, sem.at[i])
        for i, (src, dst) in enumerate(
            ((lengths_hbm, lengths), (starts_hbm, starts), (table_hbm, table), (pool_hbm, pool))
        )
    ]
    for c in copies:
        c.start()
    page_len = pool.shape[1]
    half = other.shape[0]
    me, z = idx[0], idx[1]
    column = lax.broadcasted_iota(jnp.int32, table.shape, 0)
    request = lax.broadcasted_iota(jnp.int32, table.shape, 1)
    for c in copies[:3]:
        c.wait()
    at = starts[...] + column
    here = jnp.where(at >= devices, at - devices, at) == me * groups + z
    here = here & (column * page_len < lengths[...])
    slots = jnp.where(here, table[...], 0)
    owner = request // per_owner
    chosen = []
    for flip in (1, 0):
        for m in range(half):
            chosen.append(jnp.sum(jnp.where(owner == me ^ (2 * m) ^ flip, slots, 0)))
    copies[3].wait()
    for m in range(half):
        other[m] = pool[chosen[m]]
        same[m] = pool[chosen[half + m]]


def gather_pages(idx, pool, lengths, starts, table, groups):
    requests, _ = table.shape
    owners = pool.shape[0]
    half = jax.ShapeDtypeStruct((owners // 2,) + pool.shape[1:], pool.dtype)
    cfg = (owners * groups, groups, requests // owners)
    args = (lengths.reshape(1, -1), starts.reshape(1, -1), table.T, pool)
    args = tuple(pltpu.with_memory_space_constraint(x, pltpu.HBM) for x in args)
    return pl.pallas_call(
        functools.partial(gather_kernel, cfg),
        out_shape=[half] * 2,
        in_specs=[SMEM] + [HBM] * 4,
        out_specs=[VMEM] * 2,
        scratch_shapes=[pltpu.VMEM(x.shape, x.dtype) for x in args]
        + [pltpu.SemaphoreType.DMA((4,))],
        compiler_params=pltpu.CompilerParams(vmem_limit_bytes=16 << 20),
    )(idx, *args)


def pack_kernel(same, part, ring, *outs):
    last = len(outs)
    for i, source in enumerate((same, part)):
        ring[i] = source[0]
        ring[2 + i] = source[last]
        for m, out in enumerate(outs, 1):
            out[i] = source[m]


def pack_pages(same, part):
    pair = jax.ShapeDtypeStruct((2,) + same.shape[1:], same.dtype)
    ring = jax.ShapeDtypeStruct((4,) + same.shape[1:], same.dtype)
    count = same.shape[0] - 1
    return pl.pallas_call(
        pack_kernel,
        out_shape=[ring] + [pair] * count,
        in_specs=[VMEM] * 2,
        out_specs=[VMEM] * (count + 1),
        compiler_params=pltpu.CompilerParams(vmem_limit_bytes=16 << 20),
    )(same, part)


def absorb_kernel(queries_hbm, key_up_hbm, out, queries, key_up, flat, rope, sem):
    rows, heads, dim = queries.shape
    nope, rank = key_up.shape[1:]
    pieces = sem.shape[0] - 1
    n = heads // pieces
    copies = [pltpu.make_async_copy(queries_hbm, queries, sem.at[pieces])]
    for i in range(pieces):
        at = pl.ds(i * n, n)
        copies.append(pltpu.make_async_copy(key_up_hbm.at[at], key_up.at[at], sem.at[i]))
    for c in copies:
        c.start()
    copies[0].wait()
    q = queries[...].reshape(rows * heads, dim).astype(F32)
    flat[...] = q[:, :nope]
    rope[:, : dim - nope] = q[:, nope:]
    for h in range(heads):
        if h % n == 0:
            copies[1 + h // n].wait()
        pick = pl.ds(h, rows, stride=heads)
        at = pl.ds(h * rows, rows)
        out[at, :rank] = jnp.dot(
            flat[pick, :].astype(BF16), key_up[h], preferred_element_type=F32
        ).astype(BF16)
        out[at, rank:] = rope[pick, :][:, : dim - nope].astype(BF16)


def absorb(queries, key_up):
    rows, heads, dim = queries.shape
    width = key_up.shape[2] + dim - key_up.shape[1]
    args = tuple(pltpu.with_memory_space_constraint(x, pltpu.HBM) for x in (queries, key_up))
    return pl.pallas_call(
        absorb_kernel,
        out_shape=jax.ShapeDtypeStruct((heads * rows, width), BF16),
        in_specs=[HBM] * 2,
        out_specs=VMEM,
        scratch_shapes=[
            pltpu.VMEM(queries.shape, queries.dtype),
            pltpu.VMEM(key_up.shape, key_up.dtype),
            pltpu.VMEM((rows * heads, key_up.shape[1]), F32),
            pltpu.VMEM((rows * heads, pl.cdiv(dim - key_up.shape[1], 128) * 128), F32),
            pltpu.SemaphoreType.DMA((5,)),
        ],
        compiler_params=pltpu.CompilerParams(vmem_limit_bytes=16 << 20),
        cost_estimate=pl.CostEstimate(
            flops=2 * rows * key_up.size, transcendentals=0, bytes_accessed=2 * key_up.size
        ),
    )(*args)


def row_chunks(heads, rows, most):
    size = max(1, most // rows)
    return [(h, min(size, heads - h)) for h in range(0, heads, size)]


def attend(q, parts, scale, lat_rank, old):
    n = q.shape[0]
    scores = []
    for keys, bias in parts:
        rows = bias.shape[0]
        s = lax.dot_general(q, keys, (((1,), (1,)), ((), ())), preferred_element_type=F32)
        scores.append((s.reshape(n // rows, rows, -1) * scale + bias[None]).reshape(n, -1))
    m = functools.reduce(jnp.maximum, [jnp.max(s, axis=-1, keepdims=True) for s in scores])
    if old is not None:
        m = jnp.maximum(old[0], m)
    l, acc = 0.0, 0.0
    for s, (keys, _) in zip(scores, parts):
        w = jnp.exp(s - m)
        l = l + jnp.sum(w, axis=-1, keepdims=True)
        acc = acc + jnp.dot(w.astype(BF16), keys[:, :lat_rank], preferred_element_type=F32)
    if old is not None:
        keep = jnp.exp(old[0] - m)
        l = l + old[1] * keep
        acc = acc + old[2] * keep
    return m, l, acc


def fill_bias(cfg, idx, lengths, starts, bias):
    devices, groups, per_owner, page_len = cfg
    rows, width = bias.shape[1:]
    tile = max(128, page_len)
    lane = lax.broadcasted_iota(jnp.int32, (rows, tile), 1)
    request = lax.broadcasted_iota(jnp.int32, (rows, tile), 0) // STEPS
    me = idx[0]

    def one(i, _):
        plane, t = i // (width // tile), lax.rem(i, width // tile)
        limit = jnp.zeros((rows, tile), jnp.int32)
        for p in range(tile // page_len):
            home = (me ^ (t * (tile // page_len) + p)) * groups + plane
            for r in range(per_owner):
                at = home - starts[me * per_owner + r]
                at = jnp.where(at < 0, at + devices, at)
                seen = lengths[me * per_owner + r] - (at - p) * page_len
                limit = jnp.where((request == r) & (lane // page_len == p), seen, limit)
        bias[plane, :, pl.ds(pl.multiple_of(t * tile, tile), tile)] = jnp.where(
            lane < limit, 0.0, HIDDEN
        ).astype(F32)
        return 0

    lax.fori_loop(0, groups * (width // tile), one, 0)


def stage_kernel(cfg, *rest):
    heads, rows, lat_rank, scale, counts, first, last, hops, geometry, skips = cfg
    rest = list(rest)

    def take(n):
        out = rest[:n]
        del rest[:n]
        return out

    idx, q = take(2)
    if first:
        lengths, starts, fresh = take(3)
    else:
        bias, m_in, l_in, acc_in = take(4)
    if last:
        (value_up,) = take(1)
    blocks = [list(zip(take(len(c)), c)) for c in counts]
    if last:
        (out,) = take(1)
    else:
        m_s, l_s, acc_s = take(3)
    if first:
        (bias,) = take(1)
        fill_bias(geometry, idx, lengths, starts, bias)
    groups = geometry[1]
    z = idx[1]
    parts = []
    if first:
        row = lax.broadcasted_iota(jnp.int32, (rows, rows), 0)
        col = lax.broadcasted_iota(jnp.int32, (rows, rows), 1)
        ok = (row // STEPS == col // STEPS) & (col <= row)
        parts.append((fresh[...], jnp.where(ok, 0.0, HIDDEN).astype(F32)))
    for hop, skip, block in zip(hops, skips, blocks):
        plane = lax.rem(z + groups - hop, groups)
        at = skip
        for ref, pages in block:
            n = pages * ref.shape[1]
            parts.append((ref[:pages].reshape(n, -1), bias[plane, :, at : at + n]))
            at += n
    for h, n in row_chunks(heads, rows, 256 if last else 512):
        at = pl.ds(h * rows, n * rows)
        old = None if first else (m_in[at], l_in[at], acc_in[at])
        m, l, acc = attend(q[at], parts, scale, lat_rank, old)
        if last:
            latent = (acc * (1.0 / l)).astype(BF16).reshape(n, rows, lat_rank)
            vdim = value_up.shape[-1]
            for i in range(n):
                o = jnp.dot(latent[i], value_up[h + i], preferred_element_type=F32)
                out[:, (h + i) * vdim : (h + i + 1) * vdim] = o.astype(BF16)
        else:
            m_s[at], l_s[at], acc_s[at] = m, l, acc


def stage(
    idx, q, blocks, hops, dims, geometry, fresh=None, state=None, value_up=None, skips=(0, 0)
):
    heads, rows, lat_rank, scale = dims
    first, last = fresh is not None, value_up is not None
    args, specs = [idx, q], [SMEM, VMEM]
    if first:
        args += list(fresh)
        specs += [SMEM, SMEM, VMEM]
    else:
        args += list(state)
        specs += [VMEM] * 4
    if last:
        args.append(value_up)
        specs.append(VMEM)
    for block in blocks:
        args += [x for x, _ in block]
        specs += [VMEM] * len(block)
    tokens = sum(n for _, n in blocks[0]) * geometry[3]
    total = sum(n for b in blocks for _, n in b) * geometry[3]
    if last:
        out_shape = jax.ShapeDtypeStruct((rows, heads * value_up.shape[2]), BF16)
        out_specs = VMEM
    else:
        out_shape = [
            jax.ShapeDtypeStruct((heads * rows, 1), F32),
            jax.ShapeDtypeStruct((heads * rows, 1), F32),
            jax.ShapeDtypeStruct((heads * rows, lat_rank), F32),
        ]
        if first:
            out_shape.append(jax.ShapeDtypeStruct((geometry[1], rows, tokens), F32))
        out_specs = [VMEM] * len(out_shape)
    cfg = (
        heads, rows, lat_rank, scale, tuple(tuple(n for _, n in b) for b in blocks), first, last, tuple(hops),
        geometry, skips,
    )
    work = 2 * heads * rows * total * (q.shape[1] + lat_rank)
    return pl.pallas_call(
        functools.partial(stage_kernel, cfg),
        out_shape=out_shape,
        in_specs=specs,
        out_specs=out_specs,
        compiler_params=pltpu.CompilerParams(vmem_limit_bytes=24 << 20),
        cost_estimate=pl.CostEstimate(flops=work, transcendentals=0, bytes_accessed=4 << 20),
    )(*args)


def project_kernel(masks, groups, idx, *rest):
    blocks = rest[: len(masks)]
    w = rest[len(masks)]
    outs = rest[len(masks) + 1 : len(masks) + 1 + groups]
    lhs, acc = rest[len(masks) + 1 + groups :]
    rows = blocks[0].shape[0]
    cols = w.shape[1]
    me, z = idx[0], idx[1]
    for mask, block in zip(masks, blocks):
        lhs[pl.ds(pl.multiple_of((me ^ mask) * rows, rows), rows)] = block[...]
    for c in range(0, cols, 256):
        n = min(256, cols - c)
        acc[:, c : c + n] = jnp.dot(lhs[...], w[:, c : c + n], preferred_element_type=F32)
        for j, out in enumerate(outs):
            k = out.shape[0]
            at = pl.multiple_of((z ^ j) * k, k)
            out[:, c : c + n] = acc[pl.ds(at, k), c : c + n].astype(out.dtype)


def project(idx, masks, blocks, w, groups):
    rows, depth = blocks[0].shape
    total = rows * len(blocks)
    cols = w.shape[1]
    chunk = total // groups
    outs = [jax.ShapeDtypeStruct((chunk, cols), F32 if j == 0 else BF16) for j in range(groups)]
    return pl.pallas_call(
        functools.partial(project_kernel, tuple(masks), groups),
        out_shape=outs,
        in_specs=[SMEM] + [VMEM] * (len(blocks) + 1),
        out_specs=[VMEM] * groups,
        scratch_shapes=[
            pltpu.VMEM((total, depth), BF16),
            pltpu.VMEM((total, cols), F32),
        ],
        compiler_params=pltpu.CompilerParams(vmem_limit_bytes=24 << 20),
        cost_estimate=pl.CostEstimate(
            flops=2 * total * depth * cols, transcendentals=0, bytes_accessed=2 * depth * cols
        ),
    )(idx, *blocks, w)


def swap_x(x, mask, owners):
    return lax.ppermute(x, "xfer", [(i, i ^ mask) for i in range(owners)])


def shift_z(x, k, groups):
    return lax.ppermute(x, "head", [(i, (i + k) % groups) for i in range(groups)])


def whole(
    kv_pool, lengths, start_device, page_table, queries, new_latent, key_up, value_up, out_proj
):
    owners = lax.axis_size("xfer")
    groups = lax.axis_size("head")
    page_len = kv_pool.shape[1]
    lat_rank = value_up.shape[1]
    heads = key_up.shape[0]
    rows = queries.shape[0]
    idx = jnp.stack([lax.axis_index("xfer"), lax.axis_index("head")])

    other, same = gather_pages(idx, kv_pool, lengths, start_device, page_table, groups)
    part = swap_x(other, 1, owners)
    ring, *sent, side = pack_pages(same, part)
    far = jnp.concatenate([swap_x(x, 2 * m, owners) for m, x in enumerate(sent, 1)], axis=0)
    across = owners - 2
    hops = [(ring, far, swap_x(side, across, owners))]
    for _ in range(groups - 1):
        ring = shift_z(ring, 1, groups)
        far = shift_z(far, 1, groups)
        hops.append((ring, far, swap_x(ring[2:], across, owners)))
    hops = [[(r, 2), (f, f.shape[0]), (s, 2)] for r, f, s in hops]

    q = absorb(queries, key_up)

    dims = (heads, rows, lat_rank, queries.shape[2] ** (-0.5))
    geometry = (owners * groups, groups, lengths.shape[0] // owners, page_len)
    *state, bias = stage(
        idx, q, hops[:1], (0,), dims, geometry, fresh=(lengths, start_device, new_latent)
    )
    end = groups - 1
    for t in range(1, end):
        state = stage(idx, q, [hops[t]], (t,), dims, geometry, state=[bias, *state])
    early, *late = hops[end]
    state = stage(idx, q, [[early]], (end,), dims, geometry, state=[bias, *state])
    head_out = stage(
        idx, q, [late], (end,), dims, geometry, state=[bias, *state],
        value_up=value_up, skips=(2 * page_len,),
    )

    gathered = {}
    for k in range(0, owners, 2):
        gathered[k] = swap_x(head_out, k, owners) if k else head_out
        gathered[k + 1] = swap_x(gathered[k], 1, owners)
    masks = list(range(owners))
    parts = project(idx, masks, [gathered[k] for k in masks], out_proj, groups)
    total = parts[0]
    for k in range(1, groups):
        moved = lax.ppermute(parts[k], "head", [(i, i ^ k) for i in range(groups)])
        total = total + moved.astype(F32)
    return total.astype(BF16)


def solution(mesh):
    in_specs = (
        P(("xfer", "head"), None, None),
        P(),
        P(),
        P(),
        P("xfer", "head", None),
        P("xfer", None),
        P("head", None, None),
        P("head", None, None),
        P("head", "xfer"),
    )
    out_specs = P("head", "xfer")
    return jax.shard_map(whole, mesh=mesh, in_specs=in_specs, out_specs=out_specs, check_vma=False)
```
